256 devices in a mesh: gx: 4 (over y), gy: 8 (over z_hi, core), gz: 8 (over z_lo, x).
Axes of the slice: x: 4, y: 4, z: 8 (z_hi: 4, z_lo: 2; z = z_hi * 2 + z_lo), core: 2. Of those that a mesh axis runs over, the one named last changes fastest.
Arguments:
- states: float32 [41, 32, 128, 1024], P(None, 'gz', 'gy', 'gx'), may hold values from 0 to 1
- prior_states: float32 [41, 32, 128, 1024], P(None, 'gz', 'gy', 'gx'), may hold values from 0 to 1
- cell_layers: int32 [32, 128, 1024], P('gz', 'gy', 'gx'), may hold values from 0 to 2
- fiber_classes: int32 [32, 128, 1024], P('gz', 'gy', 'gx'), may hold values from 0 to 15
- writer_stripe: int32 [64], replicated, may hold values from 0 to 63, each once
- gate_half: float32 [3, 40], replicated, may hold values from -1 to 1.5
- gate_slope: float32 [3, 40], replicated, may hold values from 1 to 8
- gate_tau: float32 [3, 40], replicated, may hold values from 1 to 40
- gate_conduct: float32 [3, 40], replicated, may hold values from 0.002 to 0.025
- gate_reversal: float32 [3, 40], replicated, may hold values from -1.5 to 1.5
- fiber_conduct: float32 [16, 3], replicated, may hold values from 0.02 to 0.15
Outputs:
- new_states: float32 [41, 32, 128, 1024], P(None, 'gz', 'gy', 'gx')
- stripes: float32 [41, 4096, 1, 1024], P(None, ('gy', 'gz'), None, 'gx')
The draws below stay inside these ranges and needn't reach their ends.
Inputs may be any that keep to these rules, and one draw needn't show every extreme that they name: `writer_stripe`: every one of the 64 stripes has exactly one writer.
All inputs are finite; a program needn't handle non-finite values.
Results may differ from the reference program's by a relative error of at most 0.000062.
Values sent between devices are 32-bit elements; how exact they have to be, the bound alone decides.
A program may use at most 64 MiB of HBM per device.

```python
import math
import jax
import jax.numpy as jnp
from jax import lax

STATES = 41
GATES = 40
LAYERS = 3
FIBERS = 16
STEPS = 4
CT = 4
CW = 16
NT = 32
NW = 128
ND = 1024
WRITERS = 64
ROWS = 1
STRIPES = 4096
N_GY = 8
N_GZ = 8


def with_ends(values, key, least, high):
    spot = [jax.random.randint(jax.random.fold_in(key, axis), (), 0, length) for axis, length in enumerate(values.shape)]
    main_axis = values.shape.index(max(values.shape))
    neighbour = spot[:main_axis] + [(spot[main_axis] + 1) % values.shape[main_axis]] + spot[main_axis + 1:]
    return values.at[tuple(spot)].set(least).at[tuple(neighbour)].set(high)


def block_levels(stream_key, dims, cuts, smallest, high):
    def one(dim, shards_of):
        heights = jax.random.uniform(jax.random.fold_in(jax.random.fold_in(stream_key, 6), dim), (shards_of,), jnp.float32, smallest / len(cuts), high / len(cuts))
        return jnp.repeat(jnp.exp(heights), dims[dim] // shards_of).reshape((-1,) + (1,) * (len(dims) - dim - 1))

    gain = one(*cuts[0])
    for cut in cuts[1:]:
        gain = gain * one(*cut)
    return gain


def setup_inputs(seed: int = 0) -> dict:
    keys = jax.random.split(jax.random.key(seed), 12)
    states = jnp.clip(1.0 * jax.random.uniform(keys[0], (STATES, NT, NW, ND), jnp.float32) ** block_levels(keys[0], (STATES, NT, NW, ND), ((1, 8), (2, 8), (3, 4)), -0.2, 0.2), 0.0, 1.0)
    prior_states = jnp.clip(1.0 * jax.random.uniform(keys[1], (STATES, NT, NW, ND), jnp.float32) ** block_levels(keys[1], (STATES, NT, NW, ND), ((1, 8), (2, 8), (3, 4)), -0.2, 0.2), 0.0, 1.0)
    cell_layers = with_ends(jax.random.randint(keys[2], (NT, NW, ND), 0, LAYERS), jax.random.fold_in(keys[2], 1), 0, LAYERS - 1).astype(jnp.int32)
    fiber_classes = with_ends(jax.random.randint(keys[3], (NT, NW, ND), 0, FIBERS), jax.random.fold_in(keys[3], 1), 0, FIBERS - 1).astype(jnp.int32)
    writer_stripe = jax.random.permutation(keys[4], WRITERS).astype(jnp.int32)
    gate_half = jnp.clip(jax.random.uniform(keys[5], (LAYERS, GATES), jnp.float32, -1.0, 1.5), -1.0, 1.5)
    gate_slope = jnp.clip(jnp.exp(jax.random.uniform(keys[6], (LAYERS, GATES), jnp.float32, math.log(1.0), math.log(8.0))), 1.0, 8.0)
    gate_tau = jnp.clip(jnp.exp(jax.random.uniform(keys[7], (LAYERS, GATES), jnp.float32, math.log(1.0), math.log(40.0))), 1.0, 40.0)
    gate_conduct = jnp.clip(jnp.exp(jax.random.uniform(keys[8], (LAYERS, GATES), jnp.float32, math.log(0.002), math.log(0.025))), 0.002, 0.025)
    gate_reversal = jnp.clip(jax.random.uniform(keys[9], (LAYERS, GATES), jnp.float32, -1.5, 1.5), -1.5, 1.5)
    fiber_conduct = jnp.clip(jax.random.uniform(keys[10], (FIBERS, 3), jnp.float32, 0.02, 0.15), 0.02, 0.15)
    return {"states": states, "prior_states": prior_states, "cell_layers": cell_layers, "fiber_classes": fiber_classes, "writer_stripe": writer_stripe, "gate_half": gate_half, "gate_slope": gate_slope, "gate_tau": gate_tau, "gate_conduct": gate_conduct, "gate_reversal": gate_reversal, "fiber_conduct": fiber_conduct}


def pick_layer(cell_layers, column):
    picked = jnp.zeros(cell_layers.shape, jnp.float32) + column[LAYERS - 1]
    for which_layer in range(LAYERS - 2, -1, -1):
        picked = jnp.where(cell_layers == which_layer, column[which_layer], picked)
    return picked


def ionic_update(voltage, gate_states, cell_layers, gate_half, gate_slope, gate_tau, gate_conduct, gate_reversal):
    def one_gate(current, inputs):
        half_row, slope_row, tau_row, cond_row, rev_row, gate_now = inputs
        steady = jax.nn.sigmoid((voltage - pick_layer(cell_layers, half_row)) * pick_layer(cell_layers, slope_row))
        decay_rate = jnp.exp(-1.0 / (pick_layer(cell_layers, tau_row) * (1.0 + steady)))
        gate_next = steady + (gate_now - steady) * decay_rate
        current = current + pick_layer(cell_layers, cond_row) * gate_next * (voltage - pick_layer(cell_layers, rev_row))
        return current, gate_next

    inputs = (gate_half.T, gate_slope.T, gate_tau.T, gate_conduct.T, gate_reversal.T, gate_states)
    current, gate_next = lax.scan(one_gate, jnp.zeros_like(voltage), inputs)
    return voltage - current, gate_next


def diffuse(excited, sigma_cells):
    padded = jnp.pad(excited, 1, mode="edge")
    centre = excited
    across = (padded[2:, 1:-1, 1:-1] - centre) + (padded[:-2, 1:-1, 1:-1] - centre)
    widthwise = (padded[1:-1, 2:, 1:-1] - centre) + (padded[1:-1, :-2, 1:-1] - centre)
    depthwise = (padded[1:-1, 1:-1, 2:] - centre) + (padded[1:-1, 1:-1, :-2] - centre)
    return excited + sigma_cells[..., 0] * across + sigma_cells[..., 1] * widthwise + sigma_cells[..., 2] * depthwise


def reference(states, prior_states, cell_layers, fiber_classes, writer_stripe, gate_half, gate_slope, gate_tau, gate_conduct, gate_reversal, fiber_conduct):
    sigma_cells = fiber_conduct[fiber_classes]
    voltage = states[0]
    gate_states = states[1:]
    for step_index in range(STEPS):
        excited, gate_states = ionic_update(voltage, gate_states, cell_layers, gate_half, gate_slope, gate_tau, gate_conduct, gate_reversal)
        voltage = diffuse(excited, sigma_cells)
    new_states = jnp.concatenate([voltage[None], gate_states], axis=0)
    blocks = prior_states.reshape(STATES, N_GZ, CT, N_GY, CW, ND)
    blocks = jnp.transpose(blocks, (0, 3, 1, 2, 4, 5)).reshape(STATES, WRITERS, WRITERS, ROWS, ND)
    chosen = jnp.take(blocks, writer_stripe, axis=2)
    stripes = jnp.transpose(chosen, (0, 2, 1, 3, 4)).reshape(STATES, STRIPES, ROWS, ND)
    return new_states, stripes
```

```python
import functools

import jax
import jax.numpy as jnp
from jax import lax
from jax.experimental import pallas as pl
from jax.experimental.pallas import tpu as pltpu
from jax.sharding import PartitionSpec as P

MESH = pl.DeviceIdType.MESH
STEPS = 4
STATES = 41
GATES = 40
LAYERS = 3
FIBERS = 16
CT, CW, CD = 4, 16, 256
ROWS = CT * CW
WRITERS = 64
GROUPS = ((1, 17), (17, 33), (33, 49), (49, 64))
LOG2E = 1.4426950408889634


def place(i):
    gy, gz = lax.axis_index("gy"), lax.axis_index("gz")
    j = lax.rem(i * 27, 64)
    z = lax.rem((gy // 2) * 2 + gz // 4 + lax.rem(j, 8), 8)
    x = lax.rem(lax.rem(gz, 4) + lax.rem(j // 8, 4), 4)
    core = lax.rem(lax.rem(gy, 2) + j // 32, 2)
    return (z // 2) * 2 + core, lax.rem(z, 2) * 4 + x


def kernel(
    states,
    prior,
    layers_in,
    fibers_in,
    writer_stripe,
    gate_half,
    gate_slope,
    gate_tau,
    gate_conduct,
    gate_reversal,
    fiber_conduct,
    new_states,
    stripes,
    held,
    send,
    layers,
    fibers,
    table,
    sigma,
    excited,
    width_out,
    across_in,
    width_in,
    depth_in,
    load_sem,
    piece_send,
    piece_recv,
    face_send,
    face_recv,
):
    gx, gy, gz = (lax.axis_index(a) for a in ("gx", "gy", "gz"))
    me = gy * 8 + gz

    def neighbour(axis, up):
        size = lax.axis_size(axis)
        return lax.rem(lax.axis_index(axis) + (1 if up else size - 1), size)

    barrier = pltpu.get_barrier_semaphore()

    def greet(i, carry):
        a, b = place(i)
        pl.semaphore_signal(barrier, inc=1, device_id={"gy": a, "gz": b}, device_id_type=MESH)
        return carry

    for up in (False, True):
        pl.semaphore_signal(
            barrier, inc=1, device_id={"gx": neighbour("gx", up)}, device_id_type=MESH
        )
    lax.fori_loop(1, WRITERS, greet, 0)

    loads = [
        pltpu.make_async_copy(states, new_states, load_sem.at[0]),
        pltpu.make_async_copy(layers_in, layers, load_sem.at[1]),
        pltpu.make_async_copy(fibers_in, fibers, load_sem.at[2]),
    ] + [
        pltpu.make_async_copy(
            prior.at[:, :, pl.ds(128 * half, 128)], held.at[:, half], load_sem.at[3 + half]
        )
        for half in range(2)
    ]
    for load in loads:
        load.start()

    def pieces(first, last):
        rows = held.reshape(STATES * 2 * ROWS, 128)

        def one(i, carry):
            a, b = place(i)
            piece = writer_stripe[a * 8 + b]
            for s in range(STATES):
                send[i, s] = rows[pl.ds(piece + s * 2 * ROWS, 2, stride=ROWS), :]
            return carry

        lax.fori_loop(first, last, one, 0)

    def own_piece():
        rows = held.reshape(STATES * 2 * ROWS, 128)
        piece = writer_stripe[me]
        for s in range(STATES):
            stripes[s, me] = rows[pl.ds(piece + s * 2 * ROWS, 2, stride=ROWS), :]

    def piece_copy(i):
        a, b = place(i)
        return pltpu.make_async_remote_copy(
            src_ref=send.at[i],
            dst_ref=stripes.at[:, me],
            send_sem=piece_send.at[i],
            recv_sem=piece_recv.at[me],
            device_id={"gy": a, "gz": b},
            device_id_type=MESH,
        )

    def send_pieces(first, last):
        def one(i, carry):
            piece_copy(i).start()
            return carry

        lax.fori_loop(first, last, one, 0)

    def face_copies(step):
        u = excited.at[step]
        plan = []
        for up in (False, True):
            side = int(up)
            plan.append((u.at[pl.ds(48 if up else 0, 16), :], across_in.at[step, side], "gz", up))
            plan.append((width_out.at[step, side], width_in.at[step, side], "gy", up))
            plan.append((u.at[:, pl.ds(128 if up else 0, 128)], depth_in.at[step, side], "gx", up))
        return [
            pltpu.make_async_remote_copy(
                src_ref=src,
                dst_ref=dst,
                send_sem=face_send.at[step * 6 + n],
                recv_sem=face_recv.at[step * 6 + n],
                device_id={axis: neighbour(axis, up)},
                device_id_type=MESH,
            )
            for n, (src, dst, axis, up) in enumerate(plan)
        ]

    def build_tables():
        def one(g, carry):
            half = [gate_half[n, g] for n in range(LAYERS)]
            slope = [gate_slope[n, g] for n in range(LAYERS)]
            tau = [gate_tau[n, g] for n in range(LAYERS)]
            conduct = [gate_conduct[n, g] for n in range(LAYERS)]
            reversal = [gate_reversal[n, g] for n in range(LAYERS)]
            for part in range(2):
                at = pl.ds(part * 32, 32)
                kind = layers[at, :]
                first, second = kind == 0, kind == 1
                for n, of in enumerate((half, slope, tau, conduct, reversal)):
                    value = jnp.where(first, of[0], jnp.where(second, of[1], of[2]))
                    if n == 1:
                        value = -value
                    if n == 2:
                        value = -1.0 / value
                    table[g, n, at, :] = value
            return carry

        lax.fori_loop(0, GATES, one, 0)
        kind = fibers[...]
        for c in range(3):
            value = jnp.full((ROWS, CD), fiber_conduct[FIBERS - 1, c], jnp.float32)
            for f in range(FIBERS - 2, -1, -1):
                value = jnp.where(kind == f, fiber_conduct[f, c], value)
            sigma[c] = value

    def ionic(step):
        for part in range(2):
            at = pl.ds(part * 32, 32)
            voltage = new_states[0, at, :]

            def one(g, current):
                grown = jnp.exp((voltage - table[g, 0, at, :]) * table[g, 1, at, :])
                steady = 1.0 / (1.0 + grown)
                decay = jnp.exp(table[g, 2, at, :] * (1.0 - 1.0 / (2.0 + grown)))
                gate = steady + (new_states[1 + g, at, :] - steady) * decay
                new_states[1 + g, at, :] = gate
                return current + table[g, 3, at, :] * gate * (voltage - table[g, 4, at, :])

            current = lax.fori_loop(0, GATES, one, jnp.zeros((32, CD), jnp.float32))
            excited[step, at, :] = voltage - current
        for t in range(CT):
            width_out[step, 0, pl.ds(t, 1), :] = excited[step, pl.ds(t * CW, 1), :]
            width_out[step, 1, pl.ds(t, 1), :] = excited[step, pl.ds(t * CW + CW - 1, 1), :]

    row = lax.broadcasted_iota(jnp.int32, (CW, CD), 0)
    lane = lax.broadcasted_iota(jnp.int32, (CW, 128), 1)
    gx_low, gx_high = gx == 0, gx == lax.axis_size("gx") - 1
    gy_low, gy_high = gy == 0, gy == lax.axis_size("gy") - 1
    gz_low, gz_high = gz == 0, gz == lax.axis_size("gz") - 1

    def diffuse(step):
        for t in range(CT):
            at = pl.ds(t * CW, CW)
            here = excited[step, at, :]
            if t == 0:
                below = jnp.where(gz_low, here, across_in[step, 1])
            else:
                below = excited[step, pl.ds((t - 1) * CW, CW), :]
            if t == CT - 1:
                above = jnp.where(gz_high, here, across_in[step, 0])
            else:
                above = excited[step, pl.ds((t + 1) * CW, CW), :]
            across = (above - here) + (below - here)

            low = jnp.broadcast_to(width_in[step, 1, pl.ds(t, 1), :], (CW, CD))
            high = jnp.broadcast_to(width_in[step, 0, pl.ds(t, 1), :], (CW, CD))
            low = jnp.where(gy_low, here, low)
            high = jnp.where(gy_high, here, high)
            below = jnp.where(row == 0, low, pltpu.roll(here, 1, 0))
            above = jnp.where(row == CW - 1, high, pltpu.roll(here, CW - 1, 0))
            widthwise = (above - here) + (below - here)

            left, right = here[:, :128], here[:, 128:]
            before = pltpu.roll(depth_in[step, 1, at, :], 1, 1)
            after = pltpu.roll(depth_in[step, 0, at, :], 127, 1)
            before = jnp.where(gx_low, left, before)
            after = jnp.where(gx_high, right, after)
            left_up, right_up = pltpu.roll(left, 1, 1), pltpu.roll(right, 1, 1)
            left_down, right_down = pltpu.roll(left, 127, 1), pltpu.roll(right, 127, 1)
            below = (jnp.where(lane == 0, before, left_up), jnp.where(lane == 0, left_up, right_up))
            above = (
                jnp.where(lane == 127, right_down, left_down),
                jnp.where(lane == 127, after, right_down),
            )
            part = excited[step, at, :] + sigma[0, at, :] * across + sigma[1, at, :] * widthwise
            for half, mid in enumerate((left, right)):
                lanes = pl.ds(128 * half, 128)
                depthwise = (above[half] - mid) + (below[half] - mid)
                new_states[0, at, lanes] = (
                    part[:, 128 * half : 128 * half + 128] + sigma[2, at, lanes] * depthwise
                )

    loads[1].wait()
    loads[2].wait()
    build_tables()
    loads[0].wait()
    ionic(0)
    loads[3].wait()
    loads[4].wait()
    pieces(*GROUPS[0])
    pl.semaphore_wait(barrier, WRITERS + 1)
    for step in range(STEPS):
        faces = face_copies(step)
        for face in faces:
            face.start()
        send_pieces(*GROUPS[step])
        if step + 1 < STEPS:
            pieces(*GROUPS[step + 1])
        else:
            own_piece()
        for face in faces:
            face.wait_recv()
        diffuse(step)
        if step + 1 < STEPS:
            ionic(step + 1)

    def drain(i, carry):
        copy = piece_copy(i)
        copy.wait_send()
        a, b = place(i)
        pltpu.make_async_remote_copy(
            src_ref=send.at[i],
            dst_ref=stripes.at[:, a * 8 + b],
            send_sem=piece_send.at[i],
            recv_sem=piece_recv.at[a * 8 + b],
            device_id={"gy": a, "gz": b},
            device_id_type=MESH,
        ).wait_recv()
        return carry

    lax.fori_loop(1, WRITERS, drain, 0)
    for step in range(STEPS):
        for face in face_copies(step):
            face.wait_send()


def per_device(
    states,
    prior_states,
    cell_layers,
    fiber_classes,
    writer_stripe,
    gate_half,
    gate_slope,
    gate_tau,
    gate_conduct,
    gate_reversal,
    fiber_conduct,
):
    f32 = jnp.float32
    anywhere = pl.BlockSpec(memory_space=pl.ANY)
    scalars = pl.BlockSpec(memory_space=pltpu.SMEM)
    vmem = pl.BlockSpec(memory_space=pltpu.VMEM)
    new_states, stripes = pl.pallas_call(
        kernel,
        out_shape=(
            jax.ShapeDtypeStruct((STATES, ROWS, CD), f32),
            jax.ShapeDtypeStruct((STATES, WRITERS, 2, 128), f32),
        ),
        in_specs=[anywhere] * 4 + [scalars] * 7,
        out_specs=(vmem, vmem),
        scratch_shapes=[
            pltpu.VMEM((STATES, 2, ROWS, 128), f32),
            pltpu.VMEM((WRITERS, STATES, 2, 128), f32),
            pltpu.VMEM((ROWS, CD), jnp.int32),
            pltpu.VMEM((ROWS, CD), jnp.int32),
            pltpu.VMEM((GATES, 5, ROWS, CD), f32),
            pltpu.VMEM((3, ROWS, CD), f32),
            pltpu.VMEM((STEPS, ROWS, CD), f32),
            pltpu.VMEM((STEPS, 2, CT, CD), f32),
            pltpu.VMEM((STEPS, 2, CW, CD), f32),
            pltpu.VMEM((STEPS, 2, CT, CD), f32),
            pltpu.VMEM((STEPS, 2, ROWS, 128), f32),
            pltpu.SemaphoreType.DMA((5,)),
            pltpu.SemaphoreType.DMA((WRITERS,)),
            pltpu.SemaphoreType.DMA((WRITERS,)),
            pltpu.SemaphoreType.DMA((STEPS * 6,)),
            pltpu.SemaphoreType.DMA((STEPS * 6,)),
        ],
        compiler_params=pltpu.CompilerParams(collective_id=0, has_side_effects=True, vmem_limit_bytes=40 * 1024 * 1024),
    )(
        states.reshape(STATES, ROWS, CD),
        prior_states.reshape(STATES, ROWS, CD),
        cell_layers.reshape(ROWS, CD),
        fiber_classes.reshape(ROWS, CD),
        writer_stripe,
        gate_half,
        gate_slope,
        gate_tau,
        gate_conduct,
        gate_reversal,
        fiber_conduct,
    )
    return new_states.reshape(states.shape), stripes.reshape(STATES, WRITERS, 1, CD)


def solution(mesh):
    cells = P(None, "gz", "gy", "gx")
    in_specs = (cells, cells, P("gz", "gy", "gx"), P("gz", "gy", "gx")) + (P(),) * 7
    out_specs = (cells, P(None, ("gy", "gz"), None, "gx"))
    return jax.shard_map(
        per_device, mesh=mesh, in_specs=in_specs, out_specs=out_specs, check_vma=False
    )
```

```python
import functools

import jax
import jax.numpy as jnp
from jax import lax
from jax.experimental import pallas as pl
from jax.experimental.pallas import tpu as pltpu
from jax.sharding import PartitionSpec as P

MESH = pl.DeviceIdType.MESH
STEPS = 4
STATES = 41
GATES = 40
LAYERS = 3
FIBERS = 16
CT, CW, CD = 4, 16, 256
ROWS = CT * CW
WRITERS = 64
CUTS = (1, 12, 23, 34, 45, 64)
LOG2E = 1.4426950408889634


def place(i):
    gy, gz = lax.axis_index("gy"), lax.axis_index("gz")
    j = lax.rem(i * 27, 64)
    z = lax.rem((gy // 2) * 2 + gz // 4 + lax.rem(j, 8), 8)
    x = lax.rem(lax.rem(gz, 4) + lax.rem(j // 8, 4), 4)
    core = lax.rem(lax.rem(gy, 2) + j // 32, 2)
    return (z // 2) * 2 + core, lax.rem(z, 2) * 4 + x


def kernel(
    states,
    prior,
    layers_in,
    fibers_in,
    writer_stripe_in,
    gate_half_in,
    gate_slope_in,
    gate_tau_in,
    gate_conduct_in,
    gate_reversal_in,
    fiber_conduct_in,
    new_states,
    stripes,
    writer_stripe,
    gate_half,
    gate_slope,
    gate_tau,
    gate_conduct,
    gate_reversal,
    fiber_conduct,
    held,
    send,
    layers,
    fibers,
    table,
    sigma,
    excited,
    width_out,
    across_in,
    width_in,
    depth_in,
    load_sem,
    piece_send,
    piece_recv,
    face_send,
    face_recv,
):
    gx, gy, gz = (lax.axis_index(a) for a in ("gx", "gy", "gz"))
    me = gy * 8 + gz

    def neighbour(axis, up):
        size = lax.axis_size(axis)
        return lax.rem(lax.axis_index(axis) + (1 if up else size - 1), size)

    barrier = pltpu.get_barrier_semaphore()

    def greet(i, carry):
        a, b = place(i)
        pl.semaphore_signal(barrier, inc=1, device_id={"gy": a, "gz": b}, device_id_type=MESH)
        return carry

    for up in (False, True):
        pl.semaphore_signal(
            barrier, inc=1, device_id={"gx": neighbour("gx", up)}, device_id_type=MESH
        )
    lax.fori_loop(1, WRITERS, greet, 0)

    def load(source, target, n):
        copy = pltpu.make_async_copy(source, target, load_sem.at[n])
        copy.start()
        return copy

    piece_loads = [load(writer_stripe_in, writer_stripe, 0)] + [
        load(prior.at[:, :, pl.ds(128 * half, 128)], held.at[:, half], 1 + half) for half in range(2)
    ]
    table_loads = [
        load(source, target, 3 + n)
        for n, (source, target) in enumerate(
            (
                (layers_in, layers),
                (gate_half_in, gate_half),
                (gate_slope_in, gate_slope),
                (gate_tau_in, gate_tau),
                (gate_conduct_in, gate_conduct),
                (gate_reversal_in, gate_reversal),
                (fibers_in, fibers),
                (fiber_conduct_in, fiber_conduct),
            )
        )
    ]
    state_load = load(states, new_states, 11)

    def pieces(first, last):
        rows = held.reshape(STATES * 2 * ROWS, 128)

        def one(i, carry):
            a, b = place(i)
            piece = writer_stripe[a * 8 + b]
            for s in range(STATES):
                send[i, s] = rows[pl.ds(piece + s * 2 * ROWS, 2, stride=ROWS), :]
            return carry

        lax.fori_loop(first, last, one, 0)

    def own_piece():
        rows = held.reshape(STATES * 2 * ROWS, 128)
        piece = writer_stripe[me]
        for s in range(STATES):
            stripes[s, me] = rows[pl.ds(piece + s * 2 * ROWS, 2, stride=ROWS), :]

    def piece_copy(i):
        a, b = place(i)
        return pltpu.make_async_remote_copy(
            src_ref=send.at[i],
            dst_ref=stripes.at[:, me],
            send_sem=piece_send.at[i],
            recv_sem=piece_recv.at[me],
            device_id={"gy": a, "gz": b},
            device_id_type=MESH,
        )

    def send_pieces(first, last):
        def one(i, carry):
            piece_copy(i).start()
            return carry

        lax.fori_loop(first, last, one, 0)

    def face_copies(step):
        u = excited.at[step]
        plan = []
        for up in (False, True):
            side = int(up)
            plan.append((u.at[pl.ds(48 if up else 0, 16), :], across_in.at[step, side], "gz", up))
            plan.append((width_out.at[step, side], width_in.at[step, side], "gy", up))
            plan.append((u.at[:, pl.ds(128 if up else 0, 128)], depth_in.at[step, side], "gx", up))
        return [
            pltpu.make_async_remote_copy(
                src_ref=src,
                dst_ref=dst,
                send_sem=face_send.at[step * 6 + n],
                recv_sem=face_recv.at[step * 6 + n],
                device_id={axis: neighbour(axis, up)},
                device_id_type=MESH,
            )
            for n, (src, dst, axis, up) in enumerate(plan)
        ]

    def build_tables():
        def one(g, carry):
            half = [gate_half[n, g] for n in range(LAYERS)]
            slope = [gate_slope[n, g] for n in range(LAYERS)]
            tau = [gate_tau[n, g] for n in range(LAYERS)]
            conduct = [gate_conduct[n, g] for n in range(LAYERS)]
            reversal = [gate_reversal[n, g] for n in range(LAYERS)]
            for part in range(2):
                at = pl.ds(part * 32, 32)
                kind = layers[at, :]
                first, second = kind == 0, kind == 1
                for n, of in enumerate((half, slope, tau, conduct, reversal)):
                    value = jnp.where(first, of[0], jnp.where(second, of[1], of[2]))
                    if n == 1:
                        value = -value
                    if n == 2:
                        value = -1.0 / value
                    table[g, n, at, :] = value
            return carry

        lax.fori_loop(0, GATES, one, 0)
        kind = fibers[...]
        for c in range(3):
            value = jnp.full((ROWS, CD), fiber_conduct[c, FIBERS - 1], jnp.float32)
            for f in range(FIBERS - 2, -1, -1):
                value = jnp.where(kind == f, fiber_conduct[c, f], value)
            sigma[c] = value

    def ionic(step):
        for part in range(2):
            at = pl.ds(part * 32, 32)
            voltage = new_states[0, at, :]

            def one(g, current):
                grown = jnp.exp((voltage - table[g, 0, at, :]) * table[g, 1, at, :])
                steady = 1.0 / (1.0 + grown)
                decay = jnp.exp(table[g, 2, at, :] * (1.0 - 1.0 / (2.0 + grown)))
                gate = steady + (new_states[1 + g, at, :] - steady) * decay
                new_states[1 + g, at, :] = gate
                return current + table[g, 3, at, :] * gate * (voltage - table[g, 4, at, :])

            current = lax.fori_loop(0, GATES, one, jnp.zeros((32, CD), jnp.float32))
            excited[step, at, :] = voltage - current
        for t in range(CT):
            width_out[step, 0, pl.ds(t, 1), :] = excited[step, pl.ds(t * CW, 1), :]
            width_out[step, 1, pl.ds(t, 1), :] = excited[step, pl.ds(t * CW + CW - 1, 1), :]

    row = lax.broadcasted_iota(jnp.int32, (CW, CD), 0)
    lane = lax.broadcasted_iota(jnp.int32, (CW, 128), 1)
    gx_low, gx_high = gx == 0, gx == lax.axis_size("gx") - 1
    gy_low, gy_high = gy == 0, gy == lax.axis_size("gy") - 1
    gz_low, gz_high = gz == 0, gz == lax.axis_size("gz") - 1

    def diffuse(step):
        for t in range(CT):
            at = pl.ds(t * CW, CW)
            here = excited[step, at, :]
            if t == 0:
                below = jnp.where(gz_low, here, across_in[step, 1])
            else:
                below = excited[step, pl.ds((t - 1) * CW, CW), :]
            if t == CT - 1:
                above = jnp.where(gz_high, here, across_in[step, 0])
            else:
                above = excited[step, pl.ds((t + 1) * CW, CW), :]
            across = (above - here) + (below - here)

            low = jnp.broadcast_to(width_in[step, 1, pl.ds(t, 1), :], (CW, CD))
            high = jnp.broadcast_to(width_in[step, 0, pl.ds(t, 1), :], (CW, CD))
            low = jnp.where(gy_low, here, low)
            high = jnp.where(gy_high, here, high)
            below = jnp.where(row == 0, low, pltpu.roll(here, 1, 0))
            above = jnp.where(row == CW - 1, high, pltpu.roll(here, CW - 1, 0))
            widthwise = (above - here) + (below - here)

            left, right = here[:, :128], here[:, 128:]
            before = pltpu.roll(depth_in[step, 1, at, :], 1, 1)
            after = pltpu.roll(depth_in[step, 0, at, :], 127, 1)
            before = jnp.where(gx_low, left, before)
            after = jnp.where(gx_high, right, after)
            left_up, right_up = pltpu.roll(left, 1, 1), pltpu.roll(right, 1, 1)
            left_down, right_down = pltpu.roll(left, 127, 1), pltpu.roll(right, 127, 1)
            below = (jnp.where(lane == 0, before, left_up), jnp.where(lane == 0, left_up, right_up))
            above = (
                jnp.where(lane == 127, right_down, left_down),
                jnp.where(lane == 127, after, right_down),
            )
            part = excited[step, at, :] + sigma[0, at, :] * across + sigma[1, at, :] * widthwise
            for half, mid in enumerate((left, right)):
                lanes = pl.ds(128 * half, 128)
                depthwise = (above[half] - mid) + (below[half] - mid)
                new_states[0, at, lanes] = (
                    part[:, 128 * half : 128 * half + 128] + sigma[2, at, lanes] * depthwise
                )

    for copy in piece_loads:
        copy.wait()
    pieces(CUTS[0], CUTS[1])
    pl.semaphore_wait(barrier, WRITERS + 1)
    send_pieces(CUTS[0], CUTS[1])
    pieces(CUTS[1], CUTS[2])
    for copy in table_loads:
        copy.wait()
    build_tables()
    state_load.wait()
    ionic(0)
    for step in range(STEPS):
        faces = face_copies(step)
        for face in faces:
            face.start()
        send_pieces(CUTS[step + 1], CUTS[step + 2])
        if step + 1 < STEPS:
            pieces(CUTS[step + 2], CUTS[step + 3])
        else:
            own_piece()
        for face in faces:
            face.wait_recv()
        diffuse(step)
        if step + 1 < STEPS:
            ionic(step + 1)

    def drain(i, carry):
        copy = piece_copy(i)
        copy.wait_send()
        a, b = place(i)
        pltpu.make_async_remote_copy(
            src_ref=send.at[i],
            dst_ref=stripes.at[:, a * 8 + b],
            send_sem=piece_send.at[i],
            recv_sem=piece_recv.at[a * 8 + b],
            device_id={"gy": a, "gz": b},
            device_id_type=MESH,
        ).wait_recv()
        return carry

    lax.fori_loop(1, WRITERS, drain, 0)
    for step in range(STEPS):
        for face in face_copies(step):
            face.wait_send()


def per_device(
    states,
    prior_states,
    cell_layers,
    fiber_classes,
    writer_stripe,
    gate_half,
    gate_slope,
    gate_tau,
    gate_conduct,
    gate_reversal,
    fiber_conduct,
):
    f32 = jnp.float32
    hbm = pl.BlockSpec(memory_space=pltpu.HBM)
    vmem = pl.BlockSpec(memory_space=pltpu.VMEM)
    new_states, stripes = pl.pallas_call(
        kernel,
        out_shape=(
            pltpu.VMEM((STATES, ROWS, CD), f32),
            pltpu.VMEM((STATES, WRITERS, 2, 128), f32),
        ),
        in_specs=[hbm] * 11,
        out_specs=(vmem, vmem),
        scratch_shapes=[
            pltpu.SMEM((WRITERS,), jnp.int32),
            pltpu.SMEM((LAYERS, GATES), f32),
            pltpu.SMEM((LAYERS, GATES), f32),
            pltpu.SMEM((LAYERS, GATES), f32),
            pltpu.SMEM((LAYERS, GATES), f32),
            pltpu.SMEM((LAYERS, GATES), f32),
            pltpu.SMEM((3, FIBERS), f32),
            pltpu.VMEM((STATES, 2, ROWS, 128), f32),
            pltpu.VMEM((WRITERS, STATES, 2, 128), f32),
            pltpu.VMEM((ROWS, CD), jnp.int32),
            pltpu.VMEM((ROWS, CD), jnp.int32),
            pltpu.VMEM((GATES, 5, ROWS, CD), f32),
            pltpu.VMEM((3, ROWS, CD), f32),
            pltpu.VMEM((STEPS, ROWS, CD), f32),
            pltpu.VMEM((STEPS, 2, CT, CD), f32),
            pltpu.VMEM((STEPS, 2, CW, CD), f32),
            pltpu.VMEM((STEPS, 2, CT, CD), f32),
            pltpu.VMEM((STEPS, 2, ROWS, 128), f32),
            pltpu.SemaphoreType.DMA((12,)),
            pltpu.SemaphoreType.DMA((WRITERS,)),
            pltpu.SemaphoreType.DMA((WRITERS,)),
            pltpu.SemaphoreType.DMA((STEPS * 6,)),
            pltpu.SemaphoreType.DMA((STEPS * 6,)),
        ],
        compiler_params=pltpu.CompilerParams(
            collective_id=0, has_side_effects=True, vmem_limit_bytes=40 * 1024 * 1024
        ),
    )(
        *(
            pltpu.with_memory_space_constraint(value, pltpu.HBM)
            for value in (
                states.reshape(STATES, ROWS, CD),
                prior_states.reshape(STATES, ROWS, CD),
                cell_layers.reshape(ROWS, CD),
                fiber_classes.reshape(ROWS, CD),
                writer_stripe,
                gate_half,
                gate_slope,
                gate_tau,
                gate_conduct,
                gate_reversal,
                fiber_conduct.T,
            )
        )
    )
    return new_states.reshape(states.shape), stripes.reshape(STATES, WRITERS, 1, CD)


def solution(mesh):
    cells = P(None, "gz", "gy", "gx")
    in_specs = (cells, cells, P("gz", "gy", "gx"), P("gz", "gy", "gx")) + (P(),) * 7
    out_specs = (cells, P(None, ("gy", "gz"), None, "gx"))
    return jax.shard_map(
        per_device, mesh=mesh, in_specs=in_specs, out_specs=out_specs, check_vma=False
    )
```

```python
import functools

import jax
import jax.numpy as jnp
from jax import lax
from jax.experimental import pallas as pl
from jax.experimental.pallas import tpu as pltpu
from jax.sharding import PartitionSpec as P

MESH = pl.DeviceIdType.MESH
STEPS = 4
STATES = 41
GATES = 40
LAYERS = 3
FIBERS = 16
CT, CW, CD = 4, 16, 256
ROWS = CT * CW
WRITERS = 64
CUTS = (1, 12, 23, 34, 45, 64)
LOG2E = 1.4426950408889634


PARTNERS = tuple((i * 27 % 64 % 8, i * 27 % 64 // 8 % 4, i * 27 % 64 // 32) for i in range(WRITERS))


def hops(partner):
    z, x, _ = PARTNERS[partner]
    return min(z, 8 - z) + min(x, 4 - x)


def kernel(
    states,
    prior,
    layers_in,
    fibers_in,
    writer_stripe_in,
    gate_half_in,
    gate_slope_in,
    gate_tau_in,
    gate_conduct_in,
    gate_reversal_in,
    fiber_conduct_in,
    new_states,
    stripes,
    writer_stripe,
    gate_half,
    gate_slope,
    gate_tau,
    gate_conduct,
    gate_reversal,
    fiber_conduct,
    chosen,
    held,
    send,
    layers,
    fibers,
    table,
    sigma,
    excited,
    width_out,
    across_in,
    width_in,
    depth_in,
    load_sem,
    piece_send,
    piece_recv,
    face_send,
    face_recv,
):
    gx, gy, gz = (lax.axis_index(a) for a in ("gx", "gy", "gz"))
    me = gy * 8 + gz

    def neighbour(axis, up):
        size = lax.axis_size(axis)
        return lax.rem(lax.axis_index(axis) + (1 if up else size - 1), size)

    layer = [lax.rem((gy // 2) * 2 + gz // 4 + k, 8) for k in range(8)]
    pair, odd = [(z // 2) * 2 for z in layer], [lax.rem(z, 2) * 4 for z in layer]
    column = [lax.rem(lax.rem(gz, 4) + k, 4) for k in range(4)]
    core = [lax.rem(gy + k, 2) for k in range(2)]

    def place(i):
        z, x, c = PARTNERS[i]
        return pair[z] + core[c], odd[z] + column[x]

    barrier = pltpu.get_barrier_semaphore()
    for i in sorted(range(1, WRITERS), key=hops, reverse=True):
        a, b = place(i)
        pl.semaphore_signal(barrier, inc=1, device_id={"gy": a, "gz": b}, device_id_type=MESH)
    for up in (False, True):
        pl.semaphore_signal(
            barrier, inc=1, device_id={"gx": neighbour("gx", up)}, device_id_type=MESH
        )

    def load(source, target, n):
        copy = pltpu.make_async_copy(source, target, load_sem.at[n])
        copy.start()
        return copy

    piece_loads = [load(writer_stripe_in, writer_stripe, 0)] + [
        load(prior.at[:, :, pl.ds(128 * half, 128)], held.at[:, half], 1 + half) for half in range(2)
    ]
    table_loads = [
        load(source, target, 3 + n)
        for n, (source, target) in enumerate(
            (
                (layers_in, layers),
                (gate_half_in, gate_half),
                (gate_slope_in, gate_slope),
                (gate_tau_in, gate_tau),
                (gate_conduct_in, gate_conduct),
                (gate_reversal_in, gate_reversal),
                (fibers_in, fibers),
                (fiber_conduct_in, fiber_conduct),
            )
        )
    ]
    state_load = load(states, new_states, 11)

    def pieces(first, last):
        rows = held.reshape(STATES * 2 * ROWS, 128)

        def one(i, carry):
            for s in range(STATES):
                send[i, s] = rows[pl.ds(chosen[i] + s * 2 * ROWS, 2, stride=ROWS), :]
            return carry

        for i in range(first, last):
            a, b = place(i)
            chosen[i] = writer_stripe[a * 8 + b]
        lax.fori_loop(first, last, one, 0)

    def own_piece():
        rows = held.reshape(STATES * 2 * ROWS, 128)
        piece = writer_stripe[me]
        for s in range(STATES):
            stripes[s, me] = rows[pl.ds(piece + s * 2 * ROWS, 2, stride=ROWS), :]

    def send_pieces(first, last):
        for i in range(first, last):
            a, b = place(i)
            pltpu.make_async_remote_copy(
                src_ref=send.at[i],
                dst_ref=stripes.at[:, me],
                send_sem=piece_send,
                recv_sem=piece_recv,
                device_id={"gy": a, "gz": b},
                device_id_type=MESH,
            ).start()

    def face_copies(step):
        u = excited.at[step]
        plan = []
        for up in (False, True):
            side = int(up)
            plan.append((u.at[pl.ds(48 if up else 0, 16), :], across_in.at[step, side], "gz", up))
            plan.append((width_out.at[step, side], width_in.at[step, side], "gy", up))
            plan.append((u.at[:, pl.ds(128 if up else 0, 128)], depth_in.at[step, side], "gx", up))
        return [
            pltpu.make_async_remote_copy(
                src_ref=src,
                dst_ref=dst,
                send_sem=face_send.at[step * 6 + n],
                recv_sem=face_recv.at[step * 6 + n],
                device_id={axis: neighbour(axis, up)},
                device_id_type=MESH,
            )
            for n, (src, dst, axis, up) in enumerate(plan)
        ]

    def build_tables():
        def one(g, carry):
            half = [gate_half[n, g] for n in range(LAYERS)]
            slope = [gate_slope[n, g] for n in range(LAYERS)]
            tau = [gate_tau[n, g] for n in range(LAYERS)]
            conduct = [gate_conduct[n, g] for n in range(LAYERS)]
            reversal = [gate_reversal[n, g] for n in range(LAYERS)]
            for part in range(2):
                at = pl.ds(part * 32, 32)
                kind = layers[at, :]
                first, second = kind == 0, kind == 1
                for n, of in enumerate((half, slope, tau, conduct, reversal)):
                    value = jnp.where(first, of[0], jnp.where(second, of[1], of[2]))
                    if n == 1:
                        value = -value
                    if n == 2:
                        value = -1.0 / value
                    table[g, n, at, :] = value
            return carry

        lax.fori_loop(0, GATES, one, 0)
        kind = fibers[...]
        for c in range(3):
            value = jnp.full((ROWS, CD), fiber_conduct[c, FIBERS - 1], jnp.float32)
            for f in range(FIBERS - 2, -1, -1):
                value = jnp.where(kind == f, fiber_conduct[c, f], value)
            sigma[c] = value

    def ionic(step):
        for part in range(2):
            at = pl.ds(part * 32, 32)
            voltage = new_states[0, at, :]

            def one(g, current):
                grown = jnp.exp((voltage - table[g, 0, at, :]) * table[g, 1, at, :])
                steady = 1.0 / (1.0 + grown)
                decay = jnp.exp(table[g, 2, at, :] * (1.0 - 1.0 / (2.0 + grown)))
                gate = steady + (new_states[1 + g, at, :] - steady) * decay
                new_states[1 + g, at, :] = gate
                return current + table[g, 3, at, :] * gate * (voltage - table[g, 4, at, :])

            current = lax.fori_loop(0, GATES, one, jnp.zeros((32, CD), jnp.float32))
            excited[step, at, :] = voltage - current
        for t in range(CT):
            width_out[step, 0, pl.ds(t, 1), :] = excited[step, pl.ds(t * CW, 1), :]
            width_out[step, 1, pl.ds(t, 1), :] = excited[step, pl.ds(t * CW + CW - 1, 1), :]

    row = lax.broadcasted_iota(jnp.int32, (CW, CD), 0)
    lane = lax.broadcasted_iota(jnp.int32, (CW, 128), 1)
    gx_low, gx_high = gx == 0, gx == lax.axis_size("gx") - 1
    gy_low, gy_high = gy == 0, gy == lax.axis_size("gy") - 1
    gz_low, gz_high = gz == 0, gz == lax.axis_size("gz") - 1

    def diffuse(step):
        for t in range(CT):
            at = pl.ds(t * CW, CW)
            here = excited[step, at, :]
            if t == 0:
                below = jnp.where(gz_low, here, across_in[step, 1])
            else:
                below = excited[step, pl.ds((t - 1) * CW, CW), :]
            if t == CT - 1:
                above = jnp.where(gz_high, here, across_in[step, 0])
            else:
                above = excited[step, pl.ds((t + 1) * CW, CW), :]
            across = (above - here) + (below - here)

            low = jnp.broadcast_to(width_in[step, 1, pl.ds(t, 1), :], (CW, CD))
            high = jnp.broadcast_to(width_in[step, 0, pl.ds(t, 1), :], (CW, CD))
            low = jnp.where(gy_low, here, low)
            high = jnp.where(gy_high, here, high)
            below = jnp.where(row == 0, low, pltpu.roll(here, 1, 0))
            above = jnp.where(row == CW - 1, high, pltpu.roll(here, CW - 1, 0))
            widthwise = (above - here) + (below - here)

            left, right = here[:, :128], here[:, 128:]
            before = pltpu.roll(depth_in[step, 1, at, :], 1, 1)
            after = pltpu.roll(depth_in[step, 0, at, :], 127, 1)
            before = jnp.where(gx_low, left, before)
            after = jnp.where(gx_high, right, after)
            left_up, right_up = pltpu.roll(left, 1, 1), pltpu.roll(right, 1, 1)
            left_down, right_down = pltpu.roll(left, 127, 1), pltpu.roll(right, 127, 1)
            below = (jnp.where(lane == 0, before, left_up), jnp.where(lane == 0, left_up, right_up))
            above = (
                jnp.where(lane == 127, right_down, left_down),
                jnp.where(lane == 127, after, right_down),
            )
            part = excited[step, at, :] + sigma[0, at, :] * across + sigma[1, at, :] * widthwise
            for half, mid in enumerate((left, right)):
                lanes = pl.ds(128 * half, 128)
                depthwise = (above[half] - mid) + (below[half] - mid)
                new_states[0, at, lanes] = (
                    part[:, 128 * half : 128 * half + 128] + sigma[2, at, lanes] * depthwise
                )

    for copy in piece_loads:
        copy.wait()
    pieces(CUTS[0], CUTS[1])
    pl.semaphore_wait(barrier, WRITERS + 1)
    send_pieces(CUTS[0], CUTS[1])
    pieces(CUTS[1], CUTS[2])
    for copy in table_loads:
        copy.wait()
    build_tables()
    state_load.wait()
    ionic(0)
    for step in range(STEPS):
        faces = face_copies(step)
        for face in faces:
            face.start()
        send_pieces(CUTS[step + 1], CUTS[step + 2])
        if step + 1 < STEPS:
            pieces(CUTS[step + 2], CUTS[step + 3])
        else:
            own_piece()
        for face in faces:
            face.wait_recv()
        diffuse(step)
        if step + 1 < STEPS:
            ionic(step + 1)

    sent = send.at[pl.ds(1, WRITERS - 1)]
    pltpu.make_async_copy(sent, sent, piece_send).wait()
    pltpu.make_async_copy(sent, sent, piece_recv).wait()
    for step in range(STEPS):
        for face in face_copies(step):
            face.wait_send()


def per_device(
    states,
    prior_states,
    cell_layers,
    fiber_classes,
    writer_stripe,
    gate_half,
    gate_slope,
    gate_tau,
    gate_conduct,
    gate_reversal,
    fiber_conduct,
):
    f32 = jnp.float32
    hbm = pl.BlockSpec(memory_space=pltpu.HBM)
    vmem = pl.BlockSpec(memory_space=pltpu.VMEM)
    new_states, stripes = pl.pallas_call(
        kernel,
        out_shape=(
            pltpu.VMEM((STATES, ROWS, CD), f32),
            pltpu.VMEM((STATES, WRITERS, 2, 128), f32),
        ),
        in_specs=[hbm] * 11,
        out_specs=(vmem, vmem),
        scratch_shapes=[
            pltpu.SMEM((WRITERS,), jnp.int32),
            pltpu.SMEM((LAYERS, GATES), f32),
            pltpu.SMEM((LAYERS, GATES), f32),
            pltpu.SMEM((LAYERS, GATES), f32),
            pltpu.SMEM((LAYERS, GATES), f32),
            pltpu.SMEM((LAYERS, GATES), f32),
            pltpu.SMEM((3, FIBERS), f32),
            pltpu.SMEM((WRITERS,), jnp.int32),
            pltpu.VMEM((STATES, 2, ROWS, 128), f32),
            pltpu.VMEM((WRITERS, STATES, 2, 128), f32),
            pltpu.VMEM((ROWS, CD), jnp.int32),
            pltpu.VMEM((ROWS, CD), jnp.int32),
            pltpu.VMEM((GATES, 5, ROWS, CD), f32),
            pltpu.VMEM((3, ROWS, CD), f32),
            pltpu.VMEM((STEPS, ROWS, CD), f32),
            pltpu.VMEM((STEPS, 2, CT, CD), f32),
            pltpu.VMEM((STEPS, 2, CW, CD), f32),
            pltpu.VMEM((STEPS, 2, CT, CD), f32),
            pltpu.VMEM((STEPS, 2, ROWS, 128), f32),
            pltpu.SemaphoreType.DMA((12,)),
            pltpu.SemaphoreType.DMA,
            pltpu.SemaphoreType.DMA,
            pltpu.SemaphoreType.DMA((STEPS * 6,)),
            pltpu.SemaphoreType.DMA((STEPS * 6,)),
        ],
        compiler_params=pltpu.CompilerParams(
            collective_id=0, has_side_effects=True, vmem_limit_bytes=40 * 1024 * 1024
        ),
    )(
        *(
            pltpu.with_memory_space_constraint(value, pltpu.HBM)
            for value in (
                states.reshape(STATES, ROWS, CD),
                prior_states.reshape(STATES, ROWS, CD),
                cell_layers.reshape(ROWS, CD),
                fiber_classes.reshape(ROWS, CD),
                writer_stripe,
                gate_half,
                gate_slope,
                gate_tau,
                gate_conduct,
                gate_reversal,
                fiber_conduct.T,
            )
        )
    )
    return new_states.reshape(states.shape), stripes.reshape(STATES, WRITERS, 1, CD)


def solution(mesh):
    cells = P(None, "gz", "gy", "gx")
    in_specs = (cells, cells, P("gz", "gy", "gx"), P("gz", "gy", "gx")) + (P(),) * 7
    out_specs = (cells, P(None, ("gy", "gz"), None, "gx"))
    return jax.shard_map(
        per_device, mesh=mesh, in_specs=in_specs, out_specs=out_specs, check_vma=False
    )
```

```python
import functools

import jax
import jax.numpy as jnp
from jax import lax
from jax.experimental import pallas as pl
from jax.experimental.pallas import tpu as pltpu
from jax.sharding import PartitionSpec as P

MESH = pl.DeviceIdType.MESH
STEPS = 4
STATES = 41
GATES = 40
LAYERS = 3
FIBERS = 16
CT, CW, CD = 4, 16, 256
ROWS = CT * CW
WRITERS = 64
CUTS = (1, 17, 28, 39, 50, 64)
LOG2E = 1.4426950408889634


NEAR = (0, 1, 7)
SPREAD = tuple((i * 27 % 64 % 8, i * 27 % 64 // 8 % 4, i * 27 % 64 // 32) for i in range(WRITERS))
PARTNERS = (
    SPREAD[:1]
    + tuple(p for p in SPREAD if p[0] in (1, 7))
    + tuple(p for p in SPREAD[1:] if p[0] not in (1, 7))
)
CHAIN = 3


def kernel(
    states,
    prior,
    layers_in,
    fibers_in,
    writer_stripe_in,
    gate_half_in,
    gate_slope_in,
    gate_tau_in,
    gate_conduct_in,
    gate_reversal_in,
    fiber_conduct_in,
    new_states,
    stripes,
    writer_stripe,
    gate_half,
    gate_slope,
    gate_tau,
    gate_conduct,
    gate_reversal,
    fiber_conduct,
    chosen,
    held,
    send,
    layers,
    fibers,
    table,
    sigma,
    excited,
    width_out,
    across_in,
    width_in,
    depth_in,
    word,
    load_sem,
    piece_send,
    piece_recv,
    face_send,
    face_recv,
):
    gx, gy, gz = (lax.axis_index(a) for a in ("gx", "gy", "gz"))
    me = gy * 8 + gz

    def neighbour(axis, up):
        size = lax.axis_size(axis)
        return lax.rem(lax.axis_index(axis) + (1 if up else size - 1), size)

    def load(source, target, n):
        copy = pltpu.make_async_copy(source, target, load_sem.at[n])
        copy.start()
        return copy

    piece_loads = [load(writer_stripe_in, writer_stripe, 0)] + [
        load(prior.at[:, :, pl.ds(128 * half, 128)], held.at[:, half], 1 + half) for half in range(2)
    ]
    table_loads = [
        load(source, target, 3 + n)
        for n, (source, target) in enumerate(
            (
                (layers_in, layers),
                (gate_half_in, gate_half),
                (gate_slope_in, gate_slope),
                (gate_tau_in, gate_tau),
                (gate_conduct_in, gate_conduct),
                (gate_reversal_in, gate_reversal),
                (fibers_in, fibers),
                (fiber_conduct_in, fiber_conduct),
            )
        )
    ]
    state_load = load(states, new_states, 11)

    layer = [lax.rem((gy // 2) * 2 + gz // 4 + k, 8) for k in range(8)]
    pair, odd = [(z // 2) * 2 for z in layer], [lax.rem(z, 2) * 4 for z in layer]
    column = [lax.rem(lax.rem(gz, 4) + k, 4) for k in range(4)]
    core = [lax.rem(gy + k, 2) for k in range(2)]

    def at(partner):
        z, x, c = partner
        return {"gy": pair[z] + core[c], "gz": odd[z] + column[x]}

    def writer(i):
        place = at(PARTNERS[i])
        return place["gy"] * 8 + place["gz"]

    barrier = pltpu.get_barrier_semaphore()
    greeted = [p for p in PARTNERS[1:] if p[0] in NEAR]
    for partner in sorted(greeted, key=lambda p: -min(p[1], 4 - p[1])):
        pl.semaphore_signal(barrier, inc=1, device_id=at(partner), device_id_type=MESH)
    for up in (False, True):
        pl.semaphore_signal(
            barrier, inc=1, device_id={"gx": neighbour("gx", up)}, device_id_type=MESH
        )

    def pass_word(n):
        for z in (1, 7):
            pl.semaphore_signal(word.at[n], inc=1, device_id=at((z, 0, 0)), device_id_type=MESH)

    def get_word(n):
        pl.semaphore_wait(word.at[n], 2)

    def pieces(first, last):
        rows = held.reshape(STATES * 2 * ROWS, 128)

        def one(i, carry):
            for s in range(STATES):
                send[i, s] = rows[pl.ds(chosen[i] + s * 2 * ROWS, 2, stride=ROWS), :]
            return carry

        for i in range(first, last):
            chosen[i] = writer_stripe[writer(i)]
        lax.fori_loop(first, last, one, 0)

    def own_piece():
        rows = held.reshape(STATES * 2 * ROWS, 128)
        piece = writer_stripe[me]
        for s in range(STATES):
            stripes[s, me] = rows[pl.ds(piece + s * 2 * ROWS, 2, stride=ROWS), :]

    def send_pieces(first, last):
        for i in range(first, last):
            pltpu.make_async_remote_copy(
                src_ref=send.at[i],
                dst_ref=stripes.at[:, me],
                send_sem=piece_send,
                recv_sem=piece_recv,
                device_id=at(PARTNERS[i]),
                device_id_type=MESH,
            ).start()

    def inner(axis, up):
        place = lax.axis_index(axis)
        return place < lax.axis_size(axis) - 1 if up else place > 0

    def faces(step, act):
        u = excited.at[step]
        plan = []
        for up in (False, True):
            side = int(up)
            plan.append((u.at[pl.ds(48 if up else 0, 16), :], across_in.at[step, side], "gz", up))
            plan.append((width_out.at[step, side], width_in.at[step, side], "gy", up))
            plan.append((u.at[:, pl.ds(128 if up else 0, 128)], depth_in.at[step, side], "gx", up))
        for n, (src, dst, axis, up) in enumerate(plan):
            copy = pltpu.make_async_remote_copy(
                src_ref=src,
                dst_ref=dst,
                send_sem=face_send.at[step * 6 + n],
                recv_sem=face_recv.at[step * 6 + n],
                device_id={axis: neighbour(axis, up)},
                device_id_type=MESH,
            )

            @pl.when(inner(axis, up != (act == "receive")))
            def _(copy=copy):
                getattr(copy, {"start": "start", "receive": "wait_recv", "end": "wait_send"}[act])()

    def build_tables():
        def one(g, carry):
            half = [gate_half[n, g] for n in range(LAYERS)]
            slope = [gate_slope[n, g] for n in range(LAYERS)]
            tau = [gate_tau[n, g] for n in range(LAYERS)]
            conduct = [gate_conduct[n, g] for n in range(LAYERS)]
            reversal = [gate_reversal[n, g] for n in range(LAYERS)]
            for part in range(2):
                at = pl.ds(part * 32, 32)
                kind = layers[at, :]
                first, second = kind == 0, kind == 1
                for n, of in enumerate((half, slope, tau, conduct, reversal)):
                    value = jnp.where(first, of[0], jnp.where(second, of[1], of[2]))
                    if n == 1:
                        value = -value
                    if n == 2:
                        value = -1.0 / value
                    table[g, n, at, :] = value
            return carry

        lax.fori_loop(0, GATES, one, 0)
        kind = fibers[...]
        for c in range(3):
            value = jnp.full((ROWS, CD), fiber_conduct[c, FIBERS - 1], jnp.float32)
            for f in range(FIBERS - 2, -1, -1):
                value = jnp.where(kind == f, fiber_conduct[c, f], value)
            sigma[c] = value

    def ionic(step):
        for part in range(2):
            at = pl.ds(part * 32, 32)
            voltage = new_states[0, at, :]

            def one(g, current):
                grown = jnp.exp((voltage - table[g, 0, at, :]) * table[g, 1, at, :])
                steady = 1.0 / (1.0 + grown)
                decay = jnp.exp(table[g, 2, at, :] * (1.0 - 1.0 / (2.0 + grown)))
                gate = steady + (new_states[1 + g, at, :] - steady) * decay
                new_states[1 + g, at, :] = gate
                return current + table[g, 3, at, :] * gate * (voltage - table[g, 4, at, :])

            current = lax.fori_loop(0, GATES, one, jnp.zeros((32, CD), jnp.float32))
            excited[step, at, :] = voltage - current
        for t in range(CT):
            width_out[step, 0, pl.ds(t, 1), :] = excited[step, pl.ds(t * CW, 1), :]
            width_out[step, 1, pl.ds(t, 1), :] = excited[step, pl.ds(t * CW + CW - 1, 1), :]

    row = lax.broadcasted_iota(jnp.int32, (CW, CD), 0)
    lane = lax.broadcasted_iota(jnp.int32, (CW, 128), 1)
    gx_low, gx_high = gx == 0, gx == lax.axis_size("gx") - 1
    gy_low, gy_high = gy == 0, gy == lax.axis_size("gy") - 1
    gz_low, gz_high = gz == 0, gz == lax.axis_size("gz") - 1

    def diffuse(step):
        for t in range(CT):
            at = pl.ds(t * CW, CW)
            here = excited[step, at, :]
            if t == 0:
                below = jnp.where(gz_low, here, across_in[step, 1])
            else:
                below = excited[step, pl.ds((t - 1) * CW, CW), :]
            if t == CT - 1:
                above = jnp.where(gz_high, here, across_in[step, 0])
            else:
                above = excited[step, pl.ds((t + 1) * CW, CW), :]
            across = (above - here) + (below - here)

            low = jnp.broadcast_to(width_in[step, 1, pl.ds(t, 1), :], (CW, CD))
            high = jnp.broadcast_to(width_in[step, 0, pl.ds(t, 1), :], (CW, CD))
            low = jnp.where(gy_low, here, low)
            high = jnp.where(gy_high, here, high)
            below = jnp.where(row == 0, low, pltpu.roll(here, 1, 0))
            above = jnp.where(row == CW - 1, high, pltpu.roll(here, CW - 1, 0))
            widthwise = (above - here) + (below - here)

            left, right = here[:, :128], here[:, 128:]
            before = pltpu.roll(depth_in[step, 1, at, :], 1, 1)
            after = pltpu.roll(depth_in[step, 0, at, :], 127, 1)
            before = jnp.where(gx_low, left, before)
            after = jnp.where(gx_high, right, after)
            left_up, right_up = pltpu.roll(left, 1, 1), pltpu.roll(right, 1, 1)
            left_down, right_down = pltpu.roll(left, 127, 1), pltpu.roll(right, 127, 1)
            below = (jnp.where(lane == 0, before, left_up), jnp.where(lane == 0, left_up, right_up))
            above = (
                jnp.where(lane == 127, right_down, left_down),
                jnp.where(lane == 127, after, right_down),
            )
            part = excited[step, at, :] + sigma[0, at, :] * across + sigma[1, at, :] * widthwise
            for half, mid in enumerate((left, right)):
                lanes = pl.ds(128 * half, 128)
                depthwise = (above[half] - mid) + (below[half] - mid)
                new_states[0, at, lanes] = (
                    part[:, 128 * half : 128 * half + 128] + sigma[2, at, lanes] * depthwise
                )

    for copy in piece_loads:
        copy.wait()
    batches = [(n, n + 4) for n in range(CUTS[0], CUTS[1], 4)]
    pieces(*batches[0])
    pl.semaphore_wait(barrier, len(greeted) + 2)
    pass_word(0)
    for n, batch in enumerate(batches):
        pieces(*(batches[n + 1] if n + 1 < len(batches) else CUTS[1:3]))
        send_pieces(*batch)
    get_word(0)
    pass_word(1)
    for copy in table_loads:
        copy.wait()
    build_tables()
    get_word(1)
    pass_word(2)
    state_load.wait()
    ionic(0)
    get_word(2)
    for step in range(STEPS):
        faces(step, "start")
        send_pieces(CUTS[step + 1], CUTS[step + 2])
        if step + 1 < STEPS:
            pieces(CUTS[step + 2], CUTS[step + 3])
        else:
            own_piece()
        faces(step, "receive")
        diffuse(step)
        if step + 1 < STEPS:
            ionic(step + 1)

    sent = send.at[pl.ds(1, WRITERS - 1)]
    pltpu.make_async_copy(sent, sent, piece_send).wait()
    pltpu.make_async_copy(sent, sent, piece_recv).wait()
    for step in range(STEPS):
        faces(step, "end")


def put_out(new_states, stripes, new_states_out, stripes_out, sem):
    copies = [
        pltpu.make_async_copy(source.at[rows], target.at[rows], sem.at[2 * n + k])
        for n, rows in enumerate((pl.ds(0, 21), pl.ds(21, 20)))
        for k, (source, target) in enumerate(((new_states, new_states_out), (stripes, stripes_out)))
    ]
    for copy in copies:
        copy.start()
    for copy in copies:
        copy.wait()


def per_device(
    states,
    prior_states,
    cell_layers,
    fiber_classes,
    writer_stripe,
    gate_half,
    gate_slope,
    gate_tau,
    gate_conduct,
    gate_reversal,
    fiber_conduct,
):
    f32 = jnp.float32
    hbm = pl.BlockSpec(memory_space=pltpu.HBM)
    vmem = pl.BlockSpec(memory_space=pltpu.VMEM)
    new_states, stripes = pl.pallas_call(
        kernel,
        out_shape=(
            pltpu.VMEM((STATES, ROWS, CD), f32),
            pltpu.VMEM((STATES, WRITERS, 2, 128), f32),
        ),
        in_specs=[hbm] * 11,
        out_specs=(vmem, vmem),
        scratch_shapes=[
            pltpu.SMEM((WRITERS,), jnp.int32),
            pltpu.SMEM((LAYERS, GATES), f32),
            pltpu.SMEM((LAYERS, GATES), f32),
            pltpu.SMEM((LAYERS, GATES), f32),
            pltpu.SMEM((LAYERS, GATES), f32),
            pltpu.SMEM((LAYERS, GATES), f32),
            pltpu.SMEM((3, FIBERS), f32),
            pltpu.SMEM((WRITERS,), jnp.int32),
            pltpu.VMEM((STATES, 2, ROWS, 128), f32),
            pltpu.VMEM((WRITERS, STATES, 2, 128), f32),
            pltpu.VMEM((ROWS, CD), jnp.int32),
            pltpu.VMEM((ROWS, CD), jnp.int32),
            pltpu.VMEM((GATES, 5, ROWS, CD), f32),
            pltpu.VMEM((3, ROWS, CD), f32),
            pltpu.VMEM((STEPS, ROWS, CD), f32),
            pltpu.VMEM((STEPS, 2, CT, CD), f32),
            pltpu.VMEM((STEPS, 2, CW, CD), f32),
            pltpu.VMEM((STEPS, 2, CT, CD), f32),
            pltpu.VMEM((STEPS, 2, ROWS, 128), f32),
            pltpu.SemaphoreType.REGULAR((CHAIN,)),
            pltpu.SemaphoreType.DMA((12,)),
            pltpu.SemaphoreType.DMA,
            pltpu.SemaphoreType.DMA,
            pltpu.SemaphoreType.DMA((STEPS * 6,)),
            pltpu.SemaphoreType.DMA((STEPS * 6,)),
        ],
        compiler_params=pltpu.CompilerParams(
            collective_id=0, has_side_effects=True, vmem_limit_bytes=40 * 1024 * 1024
        ),
    )(
        *(
            pltpu.with_memory_space_constraint(value, pltpu.HBM)
            for value in (
                states.reshape(STATES, ROWS, CD),
                prior_states.reshape(STATES, ROWS, CD),
                cell_layers.reshape(ROWS, CD),
                fiber_classes.reshape(ROWS, CD),
                writer_stripe,
                gate_half,
                gate_slope,
                gate_tau,
                gate_conduct,
                gate_reversal,
                fiber_conduct.T,
            )
        )
    )
    new_states, stripes = pl.pallas_call(
        put_out,
        out_shape=(
            jax.ShapeDtypeStruct((STATES, ROWS, CD), f32),
            jax.ShapeDtypeStruct((STATES, WRITERS, 2, 128), f32),
        ),
        in_specs=[vmem, vmem],
        out_specs=(hbm, hbm),
        scratch_shapes=[pltpu.SemaphoreType.DMA((4,))],
        compiler_params=pltpu.CompilerParams(vmem_limit_bytes=1024 * 1024),
    )(
        pltpu.with_memory_space_constraint(new_states, pltpu.VMEM),
        pltpu.with_memory_space_constraint(stripes, pltpu.VMEM),
    )
    return new_states.reshape(states.shape), stripes.reshape(STATES, WRITERS, 1, CD)


def solution(mesh):
    cells = P(None, "gz", "gy", "gx")
    in_specs = (cells, cells, P("gz", "gy", "gx"), P("gz", "gy", "gx")) + (P(),) * 7
    out_specs = (cells, P(None, ("gy", "gz"), None, "gx"))
    return jax.shard_map(
        per_device, mesh=mesh, in_specs=in_specs, out_specs=out_specs, check_vma=False
    )
```

```python
import functools

import jax
import jax.numpy as jnp
from jax import lax
from jax.experimental import pallas as pl
from jax.experimental.pallas import tpu as pltpu
from jax.sharding import PartitionSpec as P

MESH = pl.DeviceIdType.MESH
STEPS = 4
STATES = 41
GATES = 40
LAYERS = 3
FIBERS = 16
CT, CW, CD = 4, 16, 256
ROWS = CT * CW
WRITERS = 64
CUTS = (1, 18, 26, 32, 36, 42, 46, 52, 56, 64, 64)
LOG2E = 1.4426950408889634


SPREAD = tuple((i * 27 % 64 % 8, i * 27 % 64 // 8 % 4, i * 27 % 64 // 32) for i in range(WRITERS))


def steps_away(partner):
    z, x, _ = partner
    return min(z, 8 - z) + min(x, 4 - x)


GREETED = tuple(
    sorted((p for p in SPREAD[1:] if steps_away(p) < 2), key=lambda p: -min(p[0], 8 - p[0]))
)
SECOND = tuple(p for p in SPREAD if p[0] in (1, 7) and p[1] in (1, 3))
THIRD = tuple(
    p for p in SPREAD[1:] if p not in GREETED + SECOND and p[0] and steps_away(p) < 5
)[:8]
PARTNERS = (
    SPREAD[:1]
    + GREETED
    + SECOND
    + THIRD
    + tuple(p for p in SPREAD[1:] if p not in GREETED + SECOND + THIRD)
)
CHAIN = 5


def kernel(
    states,
    prior,
    layers_in,
    fibers_in,
    writer_stripe_in,
    gate_half_in,
    gate_slope_in,
    gate_tau_in,
    gate_conduct_in,
    gate_reversal_in,
    fiber_conduct_in,
    new_states,
    stripes,
    writer_stripe,
    gate_half,
    gate_slope,
    gate_tau,
    gate_conduct,
    gate_reversal,
    fiber_conduct,
    chosen,
    held,
    send,
    layers,
    fibers,
    table,
    sigma,
    excited,
    width_out,
    across_in,
    width_in,
    depth_in,
    word,
    load_sem,
    piece_send,
    piece_recv,
    face_send,
    face_recv,
):
    gx, gy, gz = (lax.axis_index(a) for a in ("gx", "gy", "gz"))
    me = gy * 8 + gz

    def neighbour(axis, up):
        size = lax.axis_size(axis)
        return lax.rem(lax.axis_index(axis) + (1 if up else size - 1), size)

    def load(source, target, n):
        copy = pltpu.make_async_copy(source, target, load_sem.at[n])
        copy.start()
        return copy

    piece_loads = [load(writer_stripe_in, writer_stripe, 0)] + [
        load(prior.at[:, :, pl.ds(128 * half, 128)], held.at[:, half], 1 + half) for half in range(2)
    ]
    table_loads = [
        load(source, target, 3 + n)
        for n, (source, target) in enumerate(
            (
                (layers_in, layers),
                (gate_half_in, gate_half),
                (gate_slope_in, gate_slope),
                (gate_tau_in, gate_tau),
                (gate_conduct_in, gate_conduct),
                (gate_reversal_in, gate_reversal),
                (fibers_in, fibers),
                (fiber_conduct_in, fiber_conduct),
            )
        )
    ]
    state_load = load(states, new_states, 11)

    layer = [lax.rem((gy // 2) * 2 + gz // 4 + k, 8) for k in range(8)]
    pair, odd = [(z // 2) * 2 for z in layer], [lax.rem(z, 2) * 4 for z in layer]
    column = [lax.rem(lax.rem(gz, 4) + k, 4) for k in range(4)]
    core = [lax.rem(gy + k, 2) for k in range(2)]

    def at(partner):
        z, x, c = partner
        return {"gy": pair[z] + core[c], "gz": odd[z] + column[x]}

    def writer(i):
        place = at(PARTNERS[i])
        return place["gy"] * 8 + place["gz"]

    barrier = pltpu.get_barrier_semaphore()
    for partner in GREETED:
        pl.semaphore_signal(barrier, inc=1, device_id=at(partner), device_id_type=MESH)
    for up in (False, True):
        pl.semaphore_signal(
            barrier, inc=1, device_id={"gx": neighbour("gx", up)}, device_id_type=MESH
        )

    beside = ((1, 0, 0), (7, 0, 0), (0, 1, 0), (0, 3, 0))

    def pass_word(n):
        for partner in beside:
            pl.semaphore_signal(word.at[n], inc=1, device_id=at(partner), device_id_type=MESH)

    def get_word(n):
        pl.semaphore_wait(word.at[n], len(beside))
        if n + 1 < CHAIN:
            pass_word(n + 1)

    def pieces(first, last):
        rows = held.reshape(STATES * 2 * ROWS, 128)

        def one(i, carry):
            for s in range(STATES):
                send[i, s] = rows[pl.ds(chosen[i] + s * 2 * ROWS, 2, stride=ROWS), :]
            return carry

        for i in range(first, last):
            chosen[i] = writer_stripe[writer(i)]
        lax.fori_loop(first, last, one, 0)

    def own_piece():
        rows = held.reshape(STATES * 2 * ROWS, 128)
        piece = writer_stripe[me]
        for s in range(STATES):
            stripes[s, me] = rows[pl.ds(piece + s * 2 * ROWS, 2, stride=ROWS), :]

    def send_pieces(first, last):
        for i in range(first, last):
            pltpu.make_async_remote_copy(
                src_ref=send.at[i],
                dst_ref=stripes.at[:, me],
                send_sem=piece_send,
                recv_sem=piece_recv,
                device_id=at(PARTNERS[i]),
                device_id_type=MESH,
            ).start()

    def inner(axis, up):
        place = lax.axis_index(axis)
        return place < lax.axis_size(axis) - 1 if up else place > 0

    def faces(step, act):
        u = excited.at[step]
        plan = []
        for up in (False, True):
            side = int(up)
            plan.append((u.at[pl.ds(48 if up else 0, 16), :], across_in.at[step, side], "gz", up))
            plan.append((width_out.at[step, side], width_in.at[step, side], "gy", up))
            plan.append((u.at[:, pl.ds(128 if up else 0, 128)], depth_in.at[step, side], "gx", up))
        for n, (src, dst, axis, up) in enumerate(plan):
            copy = pltpu.make_async_remote_copy(
                src_ref=src,
                dst_ref=dst,
                send_sem=face_send.at[step * 6 + n],
                recv_sem=face_recv.at[step * 6 + n],
                device_id={axis: neighbour(axis, up)},
                device_id_type=MESH,
            )

            @pl.when(inner(axis, up != (act == "receive")))
            def _(copy=copy):
                getattr(copy, {"start": "start", "receive": "wait_recv", "end": "wait_send"}[act])()

    def build_tables():
        def one(g, carry):
            half = [gate_half[n, g] for n in range(LAYERS)]
            slope = [gate_slope[n, g] for n in range(LAYERS)]
            tau = [gate_tau[n, g] for n in range(LAYERS)]
            conduct = [gate_conduct[n, g] for n in range(LAYERS)]
            reversal = [gate_reversal[n, g] for n in range(LAYERS)]
            for part in range(2):
                at = pl.ds(part * 32, 32)
                kind = layers[at, :]
                first, second = kind == 0, kind == 1
                for n, of in enumerate((half, slope, tau, conduct, reversal)):
                    value = jnp.where(first, of[0], jnp.where(second, of[1], of[2]))
                    if n == 1:
                        value = -value
                    if n == 2:
                        value = -1.0 / value
                    table[g, n, at, :] = value
            return carry

        lax.fori_loop(0, GATES, one, 0)
        kind = fibers[...]
        for c in range(3):
            value = jnp.full((ROWS, CD), fiber_conduct[c, FIBERS - 1], jnp.float32)
            for f in range(FIBERS - 2, -1, -1):
                value = jnp.where(kind == f, fiber_conduct[c, f], value)
            sigma[c] = value

    def ionic(step):
        for part in range(2):
            if step == 0 and part == 1:
                get_word(3)
            at = pl.ds(part * 32, 32)
            voltage = new_states[0, at, :]

            def one(g, current):
                grown = jnp.exp((voltage - table[g, 0, at, :]) * table[g, 1, at, :])
                steady = 1.0 / (1.0 + grown)
                decay = jnp.exp(table[g, 2, at, :] * (1.0 - 1.0 / (2.0 + grown)))
                gate = steady + (new_states[1 + g, at, :] - steady) * decay
                new_states[1 + g, at, :] = gate
                return current + table[g, 3, at, :] * gate * (voltage - table[g, 4, at, :])

            current = lax.fori_loop(0, GATES, one, jnp.zeros((32, CD), jnp.float32))
            excited[step, at, :] = voltage - current
        for t in range(CT):
            width_out[step, 0, pl.ds(t, 1), :] = excited[step, pl.ds(t * CW, 1), :]
            width_out[step, 1, pl.ds(t, 1), :] = excited[step, pl.ds(t * CW + CW - 1, 1), :]

    row = lax.broadcasted_iota(jnp.int32, (CW, CD), 0)
    lane = lax.broadcasted_iota(jnp.int32, (CW, 128), 1)
    gx_low, gx_high = gx == 0, gx == lax.axis_size("gx") - 1
    gy_low, gy_high = gy == 0, gy == lax.axis_size("gy") - 1
    gz_low, gz_high = gz == 0, gz == lax.axis_size("gz") - 1

    def diffuse(step):
        for t in range(CT):
            at = pl.ds(t * CW, CW)
            here = excited[step, at, :]
            if t == 0:
                below = jnp.where(gz_low, here, across_in[step, 1])
            else:
                below = excited[step, pl.ds((t - 1) * CW, CW), :]
            if t == CT - 1:
                above = jnp.where(gz_high, here, across_in[step, 0])
            else:
                above = excited[step, pl.ds((t + 1) * CW, CW), :]
            across = (above - here) + (below - here)

            low = jnp.broadcast_to(width_in[step, 1, pl.ds(t, 1), :], (CW, CD))
            high = jnp.broadcast_to(width_in[step, 0, pl.ds(t, 1), :], (CW, CD))
            low = jnp.where(gy_low, here, low)
            high = jnp.where(gy_high, here, high)
            below = jnp.where(row == 0, low, pltpu.roll(here, 1, 0))
            above = jnp.where(row == CW - 1, high, pltpu.roll(here, CW - 1, 0))
            widthwise = (above - here) + (below - here)

            left, right = here[:, :128], here[:, 128:]
            before = pltpu.roll(depth_in[step, 1, at, :], 1, 1)
            after = pltpu.roll(depth_in[step, 0, at, :], 127, 1)
            before = jnp.where(gx_low, left, before)
            after = jnp.where(gx_high, right, after)
            left_up, right_up = pltpu.roll(left, 1, 1), pltpu.roll(right, 1, 1)
            left_down, right_down = pltpu.roll(left, 127, 1), pltpu.roll(right, 127, 1)
            below = (jnp.where(lane == 0, before, left_up), jnp.where(lane == 0, left_up, right_up))
            above = (
                jnp.where(lane == 127, right_down, left_down),
                jnp.where(lane == 127, after, right_down),
            )
            part = excited[step, at, :] + sigma[0, at, :] * across + sigma[1, at, :] * widthwise
            for half, mid in enumerate((left, right)):
                lanes = pl.ds(128 * half, 128)
                depthwise = (above[half] - mid) + (below[half] - mid)
                new_states[0, at, lanes] = (
                    part[:, 128 * half : 128 * half + 128] + sigma[2, at, lanes] * depthwise
                )

    for copy in piece_loads:
        copy.wait()
    near = 1 + len(GREETED)
    pieces(CUTS[0], near)
    pl.semaphore_wait(barrier, len(GREETED) + 2)
    pass_word(0)
    pieces(near, near + 4)
    send_pieces(CUTS[0], near)
    pieces(near + 4, CUTS[1])
    get_word(0)
    send_pieces(near, near + 4)
    pieces(CUTS[1], CUTS[2])
    send_pieces(near + 4, CUTS[1])
    get_word(1)
    for copy in table_loads:
        copy.wait()
    build_tables()
    get_word(2)
    send_pieces(CUTS[1], CUTS[2])
    pieces(CUTS[2], CUTS[3])
    state_load.wait()
    ionic(0)
    get_word(4)
    for step in range(STEPS):
        faces(step, "start")
        now, half, later = CUTS[2 + 2 * step : 5 + 2 * step]
        send_pieces(now, half)
        if step + 1 < STEPS:
            pieces(half, CUTS[5 + 2 * step])
        else:
            own_piece()
        faces(step, "receive")
        diffuse(step)
        send_pieces(half, later)
        if step + 1 < STEPS:
            ionic(step + 1)

    for step in range(STEPS):
        faces(step, "end")
    sent = send.at[pl.ds(1, WRITERS - 1)]
    pltpu.make_async_copy(sent, sent, piece_send).wait()
    pltpu.make_async_copy(sent, sent, piece_recv).wait()


def put_out(new_states, stripes, new_states_out, stripes_out, sem):
    copies = [
        pltpu.make_async_copy(source.at[rows], target.at[rows], sem.at[2 * n + k])
        for n, rows in enumerate((pl.ds(0, 21), pl.ds(21, 20)))
        for k, (source, target) in enumerate(((new_states, new_states_out), (stripes, stripes_out)))
    ]
    for copy in copies:
        copy.start()
    for copy in copies:
        copy.wait()


def per_device(
    states,
    prior_states,
    cell_layers,
    fiber_classes,
    writer_stripe,
    gate_half,
    gate_slope,
    gate_tau,
    gate_conduct,
    gate_reversal,
    fiber_conduct,
):
    f32 = jnp.float32
    hbm = pl.BlockSpec(memory_space=pltpu.HBM)
    vmem = pl.BlockSpec(memory_space=pltpu.VMEM)
    new_states, stripes = pl.pallas_call(
        kernel,
        out_shape=(
            pltpu.VMEM((STATES, ROWS, CD), f32),
            pltpu.VMEM((STATES, WRITERS, 2, 128), f32),
        ),
        in_specs=[hbm] * 11,
        out_specs=(vmem, vmem),
        scratch_shapes=[
            pltpu.SMEM((WRITERS,), jnp.int32),
            pltpu.SMEM((LAYERS, GATES), f32),
            pltpu.SMEM((LAYERS, GATES), f32),
            pltpu.SMEM((LAYERS, GATES), f32),
            pltpu.SMEM((LAYERS, GATES), f32),
            pltpu.SMEM((LAYERS, GATES), f32),
            pltpu.SMEM((3, FIBERS), f32),
            pltpu.SMEM((WRITERS,), jnp.int32),
            pltpu.VMEM((STATES, 2, ROWS, 128), f32),
            pltpu.VMEM((WRITERS, STATES, 2, 128), f32),
            pltpu.VMEM((ROWS, CD), jnp.int32),
            pltpu.VMEM((ROWS, CD), jnp.int32),
            pltpu.VMEM((GATES, 5, ROWS, CD), f32),
            pltpu.VMEM((3, ROWS, CD), f32),
            pltpu.VMEM((STEPS, ROWS, CD), f32),
            pltpu.VMEM((STEPS, 2, CT, CD), f32),
            pltpu.VMEM((STEPS, 2, CW, CD), f32),
            pltpu.VMEM((STEPS, 2, CT, CD), f32),
            pltpu.VMEM((STEPS, 2, ROWS, 128), f32),
            pltpu.SemaphoreType.REGULAR((CHAIN,)),
            pltpu.SemaphoreType.DMA((12,)),
            pltpu.SemaphoreType.DMA,
            pltpu.SemaphoreType.DMA,
            pltpu.SemaphoreType.DMA((STEPS * 6,)),
            pltpu.SemaphoreType.DMA((STEPS * 6,)),
        ],
        compiler_params=pltpu.CompilerParams(
            collective_id=0, has_side_effects=True, vmem_limit_bytes=40 * 1024 * 1024
        ),
    )(
        *(
            pltpu.with_memory_space_constraint(value, pltpu.HBM)
            for value in (
                states.reshape(STATES, ROWS, CD),
                prior_states.reshape(STATES, ROWS, CD),
                cell_layers.reshape(ROWS, CD),
                fiber_classes.reshape(ROWS, CD),
                writer_stripe,
                gate_half,
                gate_slope,
                gate_tau,
                gate_conduct,
                gate_reversal,
                fiber_conduct.T,
            )
        )
    )
    new_states, stripes = pl.pallas_call(
        put_out,
        out_shape=(
            jax.ShapeDtypeStruct((STATES, ROWS, CD), f32),
            jax.ShapeDtypeStruct((STATES, WRITERS, 2, 128), f32),
        ),
        in_specs=[vmem, vmem],
        out_specs=(hbm, hbm),
        scratch_shapes=[pltpu.SemaphoreType.DMA((4,))],
        compiler_params=pltpu.CompilerParams(vmem_limit_bytes=1024 * 1024),
    )(
        pltpu.with_memory_space_constraint(new_states, pltpu.VMEM),
        pltpu.with_memory_space_constraint(stripes, pltpu.VMEM),
    )
    return new_states.reshape(states.shape), stripes.reshape(STATES, WRITERS, 1, CD)


def solution(mesh):
    cells = P(None, "gz", "gy", "gx")
    in_specs = (cells, cells, P("gz", "gy", "gx"), P("gz", "gy", "gx")) + (P(),) * 7
    out_specs = (cells, P(None, ("gy", "gz"), None, "gx"))
    return jax.shard_map(
        per_device, mesh=mesh, in_specs=in_specs, out_specs=out_specs, check_vma=False
    )
```
